32 devices in a mesh: heads: 4 (over y, x), seq: 8 (over z, core).
Axes of the slice: x: 2, y: 2, z: 4, core: 2. Of those that a mesh axis runs over, the one named last changes fastest.
Arguments:
- query: bfloat16 [24, 128, 576], P(None, 'heads'), may hold values from -1024 to 1024
- cache: bfloat16 [4096, 576], P('seq'), may hold values from -8 to 8
- segments: int32 [4096], P('seq'), may hold values from 0 to 3, as said below
- groups: int32 [24], replicated, may hold values from 0 to 3
- value_up: bfloat16 [128, 512, 128], P('heads'), may hold values from -3 to 3
- out_proj: bfloat16 [16384, 7168], P('heads', 'seq'), may hold values from -0.046875 to 0.046875
- targets: float32 [24, 7168], P(None, 'seq'), may hold values from -20 to 20
Outputs:
- projected: float32 [24, 7168], P(None, 'seq')
- loss: float32 [], replicated
- query_grad: float32 [24, 128, 576], P(None, 'heads')
- cache_grad: float32 [4096, 576], P('seq', 'heads')
The draws below stay inside these ranges and needn't reach their ends.
Inputs may be any that keep to these rules, and one draw needn't show every extreme that they name: `segments`: constant over each aligned tile of 128 cached tokens; every group number appears in some tile.
All inputs are finite; a program needn't handle non-finite values.
Results may differ from the reference program's by a relative error of at most 0.015.
Values may be sent and summed in bfloat16 or wider, within the bound.
No kernel may reach another device: no remote copies, remote signals or barrier semaphores. Data moves between devices by JAX's collectives and lax.ppermute only.
A program may use at most 64 MiB of HBM per device.

```python
import jax
import jax.numpy as jnp
from jax import lax

DMODEL = 7168
HEADS = 128
LATENT = 512
VDIM = 128
QUERIES = 24
TILE = 128
SEGS = 4
WIDTH = 576
CACHE = 4096


def layout(key):
    base = jax.random.fold_in(key, 7101)
    tile_ids = jax.random.randint(jax.random.fold_in(base, 1), (CACHE // TILE,), 0, SEGS).astype(jnp.int32)
    order = jax.random.permutation(jax.random.fold_in(base, 2), SEGS).astype(jnp.int32)
    tile_ids = tile_ids.at[:SEGS].set(order)
    groups = jax.random.randint(jax.random.fold_in(base, 3), (QUERIES,), 0, SEGS).astype(jnp.int32)
    return (tile_ids, groups)


def cache_values(key):
    raw = jnp.clip(jax.random.normal(jax.random.fold_in(key, 7202), (CACHE, WIDTH), jnp.float32), -6.0, 6.0)
    return raw


def draw_cache(key, part):
    return cache_values(key).astype(jnp.bfloat16)


def draw_query(key, part):
    queries = jnp.clip(jax.random.normal(jax.random.fold_in(key, 7303), (QUERIES, HEADS, WIDTH), jnp.float32), -6.0, 6.0)
    return queries.astype(jnp.bfloat16)


def draw_segments(key, part):
    tile_ids, groups = layout(key)
    return jnp.repeat(tile_ids, TILE).astype(jnp.int32)


def draw_groups(key, part):
    tile_ids, groups = layout(key)
    return groups


def draw_targets(key, part):
    noise = jnp.clip(jax.random.normal(jax.random.fold_in(key, 7404), (QUERIES, DMODEL), jnp.float32), -6.0, 6.0)
    ramp = jnp.arange(DMODEL, dtype=jnp.float32) / DMODEL
    scales = 0.5 * jnp.exp(ramp * jnp.log(4.0))
    return noise * scales[None, :]


def level_of(own_key, shape, shards, smallest, high):
    factor_of, own = 1.0, jax.random.fold_in(own_key, 6)
    for dim, blocks in shards:
        steps = jnp.exp(jax.random.uniform(jax.random.fold_in(own, dim), (blocks,), jnp.float32, smallest / len(shards), high / len(shards)))
        factor_of = factor_of * jnp.repeat(steps, shape[dim] // blocks).reshape([-1 if axis == dim else 1 for axis in range(len(shape))])
    return factor_of


def bell_draw(stream_key, extent, scale, reach, shards=(), held_as=jnp.bfloat16):
    drawn = jax.random.normal(stream_key, extent, jnp.float32) * scale
    if len(shards) > 0:
        drawn = level_of(stream_key, extent, shards, -0.22, 0.18) * drawn
    return jnp.clip(drawn, min=-reach, max=reach).astype(held_as)


def setup_inputs(seed: int = 0) -> dict:
    key_list = jax.random.split(jax.random.key(seed), 8)
    return {
        "query": draw_query(jax.random.fold_in(key_list[7], 71), 0),
        "cache": draw_cache(jax.random.fold_in(key_list[7], 71), 0),
        "segments": draw_segments(jax.random.fold_in(key_list[7], 71), 0),
        "groups": draw_groups(jax.random.fold_in(key_list[7], 71), 0),
        "value_up": bell_draw(key_list[4], (HEADS, LATENT, VDIM), 0.5, 3.0, ((0, 4),)),
        "out_proj": bell_draw(key_list[5], (HEADS * VDIM, DMODEL), (HEADS * VDIM) ** -0.5, 0.046875, ((0, 4), (1, 8))),
        "targets": draw_targets(jax.random.fold_in(key_list[7], 71), 0),
    }


scale_factor = 0.07216878364870322
floor_value = -1.0e30


def reference(query, cache, segments, groups, value_up, out_proj, targets):
    latent = value_up.shape[1]
    values = cache[:, :latent]
    allowed = groups[:, None] == segments[None, :]

    def head_scores(head_index):
        query_head = query[:, head_index, :]
        scores = jnp.dot(query_head, cache.T, preferred_element_type=jnp.float32) * scale_factor
        return query_head, jnp.where(allowed, scores, floor_value)

    def head_forward(head_index):
        query_head, masked = head_scores(head_index)
        maximum = jnp.max(masked, axis=1)
        weights = jnp.where(allowed, jnp.exp(masked - maximum[:, None]), 0.0)
        totals = jnp.sum(weights, axis=1)
        latent_sum = jnp.dot(weights.astype(jnp.bfloat16), values, preferred_element_type=jnp.float32)
        latent_out = (latent_sum / totals[:, None]).astype(jnp.bfloat16)
        value_out = jnp.dot(latent_out, value_up[head_index], preferred_element_type=jnp.float32).astype(jnp.bfloat16)
        return value_out, maximum, totals

    value_out, maxima, totals = lax.map(head_forward, jnp.arange(HEADS).astype(jnp.int32))
    flattened = jnp.transpose(value_out, (1, 0, 2)).reshape(QUERIES, HEADS * VDIM)
    projected = jnp.dot(flattened, out_proj, preferred_element_type=jnp.float32)
    residual = projected - targets
    loss = jnp.sum(residual * residual) / (QUERIES * DMODEL)
    d_projected = residual.astype(jnp.bfloat16)
    d_value = jnp.dot(d_projected, out_proj.T, preferred_element_type=jnp.float32).reshape(QUERIES, HEADS, VDIM)

    def head_backward(carried, head_index):
        query_head, masked = head_scores(head_index)
        probs = jnp.where(allowed, jnp.exp(masked - maxima[head_index][:, None]), 0.0) / totals[head_index][:, None]
        value_grad = d_value[:, head_index, :]
        d_latent = jnp.dot(value_grad.astype(jnp.bfloat16), value_up[head_index].T, preferred_element_type=jnp.float32).astype(jnp.bfloat16)
        row_dot = jnp.sum(value_grad * value_out[head_index].astype(jnp.float32), axis=1)
        d_probs = jnp.dot(d_latent, values.T, preferred_element_type=jnp.float32)
        d_scores = (scale_factor * probs * (d_probs - row_dot[:, None])).astype(jnp.bfloat16)
        query_part = jnp.dot(d_scores, cache, preferred_element_type=jnp.float32)
        key_part = jnp.dot(d_scores.T, query_head, preferred_element_type=jnp.float32)
        value_part = jnp.dot(probs.astype(jnp.bfloat16).T, d_latent, preferred_element_type=jnp.float32)
        padding = jnp.zeros((value_part.shape[0], key_part.shape[1] - latent), jnp.float32)
        return carried + key_part + jnp.concatenate([value_part, padding], axis=1), query_part

    start_grad = jnp.zeros((CACHE, WIDTH), jnp.float32)
    cache_grad, query_parts = lax.scan(head_backward, start_grad, jnp.arange(HEADS).astype(jnp.int32))
    query_grad = jnp.transpose(query_parts, (1, 0, 2))
    return projected, loss, query_grad, cache_grad
```

```python
import jax
import jax.numpy as jnp
from jax import lax
from jax.sharding import PartitionSpec as P

scale_factor = 0.07216878364870322
floor_value = -1e30
bf16 = jnp.bfloat16
f32 = jnp.float32


def stages_of(size, first=1):
    stages, stride = [], first
    while stride < size:
        left = size // stride
        radix = 4 if left % 4 == 0 else 2
        stages.append((stride, radix))
        stride *= radix
    return stages


def digit(axis, stage):
    stride, radix = stage
    return (lax.axis_index(axis) // stride) % radix


def swap(x, axis, stage, k):
    stride = stage[0]
    n = lax.axis_size(axis)
    return lax.ppermute(x, axis, [(i, i ^ (k * stride)) for i in range(n)])


def swap_all(x, axis, stage):
    got = {k: swap(x, axis, stage, k) for k in range(stage[1] - 1, 0, -1)}
    return [x] + [got[k] for k in range(1, stage[1])]


def pick(x, index):
    return lax.dynamic_index_in_dim(x, index, 0, keepdims=False)


def ordered(parts, d):
    stacked = jnp.stack(parts, 0)
    return jnp.stack([pick(stacked, d ^ j) for j in range(len(parts))], 0)


def scatter_sum(x, axis, stage):
    d = digit(axis, stage)
    got = {}
    for k in range(stage[1] - 1, 0, -1):
        got[k] = swap(pick(x, d ^ k), axis, stage, k)
    total = pick(x, d).astype(f32)
    for k in got:
        total = total + got[k].astype(f32)
    return total.astype(bf16)


def gather(x, axis, stage):
    return ordered(swap_all(x, axis, stage), digit(axis, stage))


def sum_all(x, axis, stage):
    parts = swap_all(x, axis, stage)
    total = parts[0].astype(f32)
    for p in parts[1:]:
        total = total + p.astype(f32)
    return total.astype(bf16)


def combine(parts):
    top = parts[0][1]
    for p in parts[1:]:
        top = jnp.maximum(top, p[1])
    mass = [p[2] * jnp.exp(p[1] - top) for p in parts]
    total = mass[0]
    for w in mass[1:]:
        total = total + w
    inverse = 1.0 / jnp.maximum(total, 1e-30)
    value = sum((w * inverse)[..., None] * p[0].astype(f32) for w, p in zip(mass, parts))
    return value.astype(bf16), top, total


def on_device(query, cache, segments, groups, value_up, out_proj, targets):
    query_len, head_count, width = query.shape
    latent, vwidth = value_up.shape[1], value_up.shape[2]
    rows = query_len * head_count
    cache_len = cache.shape[0]
    values = cache[:, :latent]
    seq_stages = stages_of(lax.axis_size("seq"), 2)
    head_stages = stages_of(lax.axis_size("heads"))
    pair = (1, 2)
    query_rows = jnp.transpose(query, (1, 0, 2)).reshape(rows, width)
    allowed = groups[:, None] == segments[None, :]
    allowed = jnp.broadcast_to(allowed[None], (head_count, query_len, cache_len)).reshape(rows, cache_len)
    scores = jnp.einsum("rc,tc->rt", query_rows, cache, preferred_element_type=f32) * scale_factor
    masked = jnp.where(allowed, scores, floor_value)
    local_top = jnp.max(masked, axis=1)
    weights = jnp.where(allowed, jnp.exp(masked - local_top[:, None]), 0.0)
    local_total = jnp.sum(weights, axis=1)
    mixed = jnp.dot(weights.astype(bf16), values, preferred_element_type=f32)
    mixed = (mixed / jnp.maximum(local_total, 1e-30)[:, None]).astype(bf16)
    value = jnp.einsum(
        "hqc,hcv->hqv",
        mixed.reshape(head_count, query_len, latent),
        value_up,
        preferred_element_type=f32,
    ).astype(bf16)
    half = head_count // 2
    value = value.reshape(2, half, query_len, vwidth)
    stats = jnp.stack([local_top, local_total], 0).reshape(2, 2, half, query_len)
    stats = jnp.transpose(stats, (1, 0, 2, 3))
    core = digit("seq", pair)
    got = (swap(pick(value, 1 - core), "seq", pair, 1), swap(pick(stats, 1 - core), "seq", pair, 1))
    own = (pick(value, core), pick(stats, core))
    state = combine([(v, s[0], s[1]) for v, s in (own, got)])
    for stage in seq_stages:
        vs = swap_all(state[0], "seq", stage)
        ss = swap_all(jnp.stack([state[1], state[2]], 0), "seq", stage)
        state = combine([(v, s[0], s[1]) for v, s in zip(vs, ss)])
    value_out = gather(state[0], "seq", pair).reshape(head_count, query_len, vwidth)
    stats = gather(jnp.stack([state[1], state[2]], 0), "seq", pair)
    top = stats[:, 0].reshape(rows)
    totals = stats[:, 1].reshape(rows)
    projected = jnp.einsum(
        "hqv,hvd->qd",
        value_out,
        out_proj.reshape(head_count, vwidth, out_proj.shape[1]),
        preferred_element_type=f32,
    )
    for stage in head_stages:
        parts = swap_all(projected, "heads", stage)
        d = digit("heads", stage)
        stacked = jnp.stack(parts, 0)
        projected = sum(pick(stacked, d ^ j) for j in range(stage[1]))
    residual = projected - targets
    square = jnp.sum(residual * residual).reshape(1, 1)
    model_width = targets.shape[1] * lax.axis_size("seq")
    d_projected = residual.astype(bf16)
    d_value = jnp.einsum(
        "qd,hvd->hqv",
        d_projected,
        out_proj.reshape(head_count, vwidth, out_proj.shape[1]),
        preferred_element_type=f32,
    ).astype(bf16)
    d_half = scatter_sum(d_value.reshape(2, half, query_len, vwidth), "seq", pair)
    for stage in seq_stages:
        d_half = sum_all(d_half, "seq", stage)
    d_value = gather(d_half, "seq", pair).reshape(head_count, query_len, vwidth)
    for stage in [pair] + seq_stages:
        parts = swap_all(square, "seq", stage)
        d = digit("seq", stage)
        stacked = jnp.stack(parts, 0)
        square = sum(pick(stacked, d ^ j) for j in range(stage[1]))
    loss = square[0, 0] / (query_len * model_width)
    d_latent = (
        jnp.einsum("hqv,hcv->hqc", d_value, value_up, preferred_element_type=f32)
        .astype(bf16)
        .reshape(rows, latent)
    )
    row_dot = jnp.sum(d_value.astype(f32) * value_out.astype(f32), axis=2).reshape(rows)
    factor = jnp.exp(local_top - top) / totals
    probs = weights * factor[:, None]
    d_probs = jnp.einsum("rc,tc->rt", d_latent, values, preferred_element_type=f32)
    d_scores = (scale_factor * probs * (d_probs - row_dot[:, None])).astype(bf16)
    query_part = jnp.dot(d_scores, cache, preferred_element_type=f32).astype(bf16)
    piece = query_part.reshape(2, rows // 2, width)
    piece = scatter_sum(piece, "seq", pair)
    for stage in seq_stages:
        piece = piece.reshape((stage[1], piece.shape[0] // stage[1], width))
        piece = scatter_sum(piece, "seq", stage)
    for stage in seq_stages[::-1]:
        piece = gather(piece, "seq", stage).reshape(-1, width)
    piece = gather(piece, "seq", pair).reshape(head_count, query_len, width)
    query_grad = jnp.transpose(piece, (1, 0, 2)).astype(f32)
    key_part = jnp.einsum("rt,rc->tc", d_scores, query_rows, preferred_element_type=f32)
    value_part = jnp.einsum("rt,rc->tc", probs.astype(bf16), d_latent, preferred_element_type=f32)
    cache_part = key_part + jnp.concatenate(
        [value_part, jnp.zeros((cache_len, width - latent), f32)], axis=1
    )
    cache_part = cache_part.astype(bf16)
    for stage in head_stages[::-1]:
        columns = cache_part.shape[1] // stage[1]
        pieces = jnp.stack([cache_part[:, j * columns : (j + 1) * columns] for j in range(stage[1])], 0)
        cache_part = scatter_sum(pieces, "heads", stage)
    return projected, loss, query_grad, cache_part.astype(f32)


def solution(mesh):
    in_specs = (
        P(None, "heads", None),
        P("seq", None),
        P("seq"),
        P(),
        P("heads", None, None),
        P("heads", "seq"),
        P(None, "seq"),
    )
    out_specs = (P(None, "seq"), P(), P(None, "heads", None), P("seq", "heads"))
    return jax.shard_map(
        on_device, mesh=mesh, in_specs=in_specs, out_specs=out_specs, check_vma=False
    )
```

```python
import functools

import jax
import jax.numpy as jnp
from jax import lax
from jax.experimental import pallas as pl
from jax.experimental.pallas import tpu as pltpu
from jax.sharding import PartitionSpec as P

scale_factor = 0.07216878364870322
floor_value = -1e30
tiny = 1e-30
lanes = 128
waiting = 8_000_000_000
bf16 = jnp.bfloat16
f32 = jnp.float32
NT = (((1,), (1,)), ((), ()))


def stages_of(size, first=1):
    stages, stride = [], first
    while stride < size:
        left = size // stride
        radix = 4 if left % 4 == 0 else 2
        stages.append((stride, radix))
        stride *= radix
    return stages


def digit(axis, stage):
    stride, radix = stage
    return (lax.axis_index(axis) // stride) % radix


def swap(x, axis, stage, k):
    stride = stage[0]
    n = lax.axis_size(axis)
    return lax.ppermute(x, axis, [(i, i ^ (k * stride)) for i in range(n)])


def swap_all(x, axis, stage):
    got = {k: swap(x, axis, stage, k) for k in range(stage[1] - 1, 0, -1)}
    return [x] + [got[k] for k in range(1, stage[1])]


def pick(x, index):
    return lax.dynamic_index_in_dim(x, index, 0, keepdims=False)


def ordered(parts, d):
    stacked = jnp.stack(parts, 0)
    return jnp.stack([pick(stacked, d ^ j) for j in range(len(parts))], 0)


def scatter_sum(x, axis, stage):
    d = digit(axis, stage)
    got = {}
    for k in range(stage[1] - 1, 0, -1):
        got[k] = swap(pick(x, d ^ k), axis, stage, k)
    total = pick(x, d).astype(f32)
    for k in got:
        total = total + got[k].astype(f32)
    return total.astype(bf16)


def gather(x, axis, stage):
    return ordered(swap_all(x, axis, stage), digit(axis, stage))


def call(kernel, out_shape, *args, scratch=(), specs=None, flops=0, grant=4 << 20):
    moved = sum(a.size * a.dtype.itemsize for a in args)
    vmem = pl.BlockSpec(memory_space=pltpu.VMEM)
    return pl.pallas_call(
        kernel,
        out_shape=out_shape,
        in_specs=specs or [vmem] * len(args),
        out_specs=jax.tree.map(lambda _: vmem, out_shape),
        scratch_shapes=list(scratch),
        cost_estimate=pl.CostEstimate(flops=flops, bytes_accessed=moved, transcendentals=0),
        compiler_params=pltpu.CompilerParams(vmem_limit_bytes=grant),
    )(*args)


def split3(x):
    high = x.astype(bf16).astype(f32)
    rest = x - high
    middle = rest.astype(bf16).astype(f32)
    return high, middle, (rest - middle).astype(bf16).astype(f32)


def pack(top, total, heads):
    slab = jnp.zeros(top.shape, f32)
    for i, part in enumerate(split3(top) + split3(total)):
        slab = slab + (pltpu.roll(part, i * heads, 1) if i else part)
    return slab.astype(bf16)


def unpack(slab, heads):
    x = slab.astype(f32)
    s = x + pltpu.roll(x, lanes - heads, 1) + pltpu.roll(x, lanes - 2 * heads, 1)
    keep = lax.broadcasted_iota(jnp.int32, x.shape, 1) < heads
    top = jnp.where(keep, s, 0.0)
    total = jnp.where(keep, pltpu.roll(s, lanes - 3 * heads, 1), 0.0)
    return top, total


def choose(first, a, b):
    return jnp.where(first, a.astype(f32), b.astype(f32))


def forward_kernel(q_ref, cache_ref, seg_ref, grp_ref, up_hbm, own_ref, other_ref, w_ref, stat_ref, rows_ref, up_ref, mix_ref, pay_ref, sem):
    head_count, latent, _ = up_ref.shape
    query_len = grp_ref.shape[0]
    half = head_count // 2
    block = half // 2
    load = pltpu.make_async_copy(up_hbm, up_ref, sem)
    load.start()
    allowed = grp_ref[...] == seg_ref[...]
    lane = lax.broadcasted_iota(jnp.int32, (query_len, lanes), 1)
    zero = jnp.zeros((query_len, lanes), f32)
    grid = (query_len, query_len * head_count)
    offset = lax.broadcasted_iota(jnp.int32, grid, 1) - head_count * lax.broadcasted_iota(jnp.int32, grid, 0)
    stats = [[zero, zero], [zero, zero]]
    for b in range(head_count // block):
        first = b * block * query_len
        size = block * query_len
        take = [jnp.where(offset == b * block + j, 1.0, 0.0).astype(bf16) for j in range(block)]
        moved = jnp.dot(jnp.concatenate(take, axis=0), q_ref[...], preferred_element_type=f32).astype(bf16)
        rows_ref[first : first + size, :] = moved
        scores = lax.dot_general(moved, cache_ref[...], NT, preferred_element_type=f32)
        inverse = []
        for j in range(block):
            h = b * block + j
            p, at = divmod(h, half)
            s = jnp.where(allowed, scores[j * query_len : (j + 1) * query_len, :] * scale_factor, floor_value)
            top = jnp.max(s, axis=1, keepdims=True)
            w = jnp.where(allowed, jnp.exp(s - top), 0.0)
            total = jnp.sum(w, axis=1, keepdims=True)
            w_ref[h * query_len : (h + 1) * query_len, :] = w
            stats[p][0] = jnp.where(lane == at, top, stats[p][0])
            stats[p][1] = jnp.where(lane == at, total, stats[p][1])
            inverse.append(1.0 / jnp.maximum(total, tiny))
        mixed = jnp.dot(
            w_ref[first : first + size, :].astype(bf16), cache_ref[:, :latent], preferred_element_type=f32
        )
        for j in range(block):
            mix_ref[b * block + j] = (mixed[j * query_len : (j + 1) * query_len, :] * inverse[j]).astype(bf16)
    for p in range(2):
        stat_ref[p, 0] = stats[p][0]
        stat_ref[p, 1] = stats[p][1]
        pay_ref[p, half] = pack(stats[p][0], stats[p][1], half)
    load.wait()
    for h in range(head_count):
        p, at = divmod(h, half)
        pay_ref[p, at] = jnp.dot(mix_ref[h], up_ref[h], preferred_element_type=f32).astype(bf16)
    core = lax.axis_index("seq") % 2
    own_ref[...] = pay_ref[core]
    other_ref[...] = pay_ref[1 - core]


def combine_kernel(*refs):
    parts, out_ref = refs[:-1], refs[-1]
    heads = out_ref.shape[0] - 1
    stats = [unpack(r[heads], heads) for r in parts]
    top = functools.reduce(jnp.maximum, [s[0] for s in stats])
    mass = [s[1] * jnp.exp(s[0] - top) for s in stats]
    total = functools.reduce(jnp.add, mass)
    inverse = 1.0 / jnp.maximum(total, tiny)
    share = [m * inverse for m in mass]
    for h in range(heads):
        v = share[0][:, h : h + 1] * parts[0][h].astype(f32)
        for s, r in zip(share[1:], parts[1:]):
            v = v + s[:, h : h + 1] * r[h].astype(f32)
        out_ref[h] = v.astype(bf16)
    out_ref[heads] = pack(top, total, heads)


def in_order(parts, d, index=None):
    vals = [(r[...] if index is None else r[index]).astype(f32) for r in parts]
    out = []
    for j in range(len(parts)):
        k = d ^ j
        v = vals[0]
        for i in range(1, len(parts)):
            v = jnp.where(k == i, vals[i], v)
        out.append(v)
    return out


def project_kernel(val_ref, val_got_ref, proj_ref, part_ref, row_ref):
    half = val_ref.shape[0] - 1
    vwidth = val_ref.shape[2]
    low = lax.axis_index("seq") % 2 == 0
    for at in range(half):
        a = choose(low, val_ref[at], val_got_ref[at]).astype(bf16)
        b = choose(low, val_got_ref[at], val_ref[at]).astype(bf16)
        row_ref[:, at * vwidth : (at + 1) * vwidth] = a
        row_ref[:, (half + at) * vwidth : (half + at + 1) * vwidth] = b
    total = jnp.zeros(part_ref.shape, f32)
    depth = proj_ref.shape[0]
    step = 4 * vwidth if half % 2 == 0 else 2 * vwidth
    for k in range(0, depth, step):
        total = total + jnp.dot(row_ref[:, k : k + step], proj_ref[k : k + step, :], preferred_element_type=f32)
    part_ref[...] = total.astype(bf16)


def residual_kernel(stage, *refs):
    parts, (target_ref, w_ref, proj_ref, own_ref, other_ref, pay_ref) = refs[:-6], refs[-6:]
    projected = functools.reduce(jnp.add, in_order(parts, digit("heads", stage)))
    proj_ref[...] = projected
    residual = projected - target_ref[...]
    square = residual * residual
    rows, columns = square.shape
    tile = jnp.zeros((8, lanes), f32)
    for i in range(rows // 8):
        for j in range(columns // lanes):
            tile = tile + square[i * 8 : (i + 1) * 8, j * lanes : (j + 1) * lanes]
        if columns % lanes:
            left = square[i * 8 : (i + 1) * 8, columns - columns % lanes :]
            tile = tile + jnp.concatenate([left, jnp.zeros((8, lanes - columns % lanes), f32)], axis=1)
    half, vwidth = pay_ref.shape[1] - 1, pay_ref.shape[3]
    slab = jnp.concatenate(split3(tile), axis=0).astype(bf16)
    d_projected = residual.astype(bf16)
    group = 4 if half % 4 == 0 else 1
    for p in range(2):
        pay_ref[p, half] = slab
        for at in range(0, half, group):
            first = (p * half + at) * vwidth
            d = lax.dot_general(
                d_projected, w_ref[first : first + group * vwidth, :], NT, preferred_element_type=f32
            )
            for j in range(group):
                pay_ref[p, at + j] = d[:, j * vwidth : (j + 1) * vwidth].astype(bf16)
    core = lax.axis_index("seq") % 2
    own_ref[...] = pay_ref[core]
    other_ref[...] = pay_ref[1 - core]


def partial_sum_kernel(*refs):
    parts, out_ref = refs[:-1], refs[-1]
    total = parts[0][...].astype(f32)
    for r in parts[1:]:
        total = total + r[...].astype(f32)
    out_ref[...] = total.astype(bf16)


def sum_kernel(stage, *refs):
    parts, out_ref = refs[:-1], refs[-1]
    last = out_ref.shape[0] - 1
    for h in range(last):
        total = parts[0][h].astype(f32)
        for r in parts[1:]:
            total = total + r[h].astype(f32)
        out_ref[h] = total.astype(bf16)
    tiles = [s[:8] + s[8:16] + s[16:24] for s in in_order(parts, digit("seq", stage), last)]
    out_ref[last] = jnp.concatenate(split3(functools.reduce(jnp.add, tiles)), axis=0).astype(bf16)


def backward_kernel(chunk, dv_ref, dv_got_ref, val_ref, val_got_ref, w_ref, stat_ref, cache_ref, up_ref, qg_ref, ds_ref, probs_ref, dl_ref):
    _, latent, _ = up_ref.shape
    half = dv_ref.shape[0] - 1
    query_len = dv_ref.shape[1]
    count = ds_ref.shape[0]
    width = cache_ref.shape[1]
    block = 8
    low = lax.axis_index("seq") % 2 == 0
    own_stats = unpack(val_ref[half], half)
    got_stats = unpack(val_got_ref[half], half)
    factors = []
    for p in range(2):
        mine = low if p == 0 else jnp.logical_not(low)
        top = jnp.where(mine, own_stats[0], got_stats[0])
        total = jnp.where(mine, own_stats[1], got_stats[1])
        factors.append(jnp.exp(stat_ref[p, 0] - top) / jnp.maximum(total, tiny))
    size = block * query_len
    grid = (block, size)
    offset = lax.broadcasted_iota(jnp.int32, grid, 1) - query_len * lax.broadcasted_iota(jnp.int32, grid, 0)
    take = [jnp.where(offset == q, 1.0, 0.0).astype(bf16) for q in range(query_len)]
    turn = jnp.concatenate(take, axis=0)
    span = query_len // 4
    lines = span * block
    full = width - width % lanes
    for b in range(count // block):
        dots = []
        for j in range(block):
            n = b * block + j
            h = chunk * count + n
            p, at = divmod(h, half)
            mine = low if p == 0 else jnp.logical_not(low)
            dv = choose(mine, dv_ref[at], dv_got_ref[at])
            val = choose(mine, val_ref[at], val_got_ref[at])
            dots.append(jnp.sum(dv * val, axis=1, keepdims=True))
            dl = lax.dot_general(dv.astype(bf16), up_ref[h], NT, preferred_element_type=f32)
            dl_ref[n] = dl.astype(bf16)
        dlb = dl_ref[b * block : (b + 1) * block].reshape(size, latent)
        d_probs = lax.dot_general(dlb, cache_ref[:, :latent], NT, preferred_element_type=f32)
        for j in range(block):
            n = b * block + j
            h = chunk * count + n
            p, at = divmod(h, half)
            rows = slice(h * query_len, (h + 1) * query_len)
            probs = w_ref[rows, :] * factors[p][:, at : at + 1]
            probs_ref[n] = probs.astype(bf16)
            d = d_probs[j * query_len : (j + 1) * query_len, :] - dots[j]
            ds_ref[n] = (scale_factor * probs * d).astype(bf16)
        dsb = ds_ref[b * block : (b + 1) * block].reshape(size, cache_ref.shape[0])
        qg = jnp.dot(dsb, cache_ref[...], preferred_element_type=f32).astype(bf16)
        qg = jnp.dot(turn, qg, preferred_element_type=f32)
        for g in range(4):
            x = qg[g * lines : (g + 1) * lines, :]
            to = qg_ref.at[g // 2, b * 2 + g % 2]
            for c in range(full // lanes):
                to[c * lines : (c + 1) * lines, :] = x[:, c * lanes : (c + 1) * lanes].astype(bf16)
            last = jnp.concatenate([x[: lines // 2, full:], x[lines // 2 :, full:]], axis=1)
            to[(full // lanes) * lines :, :] = last.astype(bf16)


def final_kernel(stage, chunks, *refs):
    out_ref = refs[-1]
    count = stage[1]
    core = lax.axis_index("seq") % 2
    d = digit("seq", stage)
    query_len, _, width = out_ref.shape
    block = 8
    span = query_len // 4
    lines = span * block
    full = width - width % lanes
    left = width - full
    unit = lines * width // lanes
    at = 0
    for chunk in range(chunks):
        for half in (core, 1 - core):
            for k in range(count):
                ref = refs[at]
                at += 1
                held = ref.shape[0] // unit
                for u in range(held):
                    index = (d ^ k) * held + u
                    first = half * 2 * span + lax.rem(index, 2) * span
                    head = pl.multiple_of((chunk * held * count // 2 + index // 2) * block, block)
                    for q in range(span):
                        to = out_ref.at[first + q, pl.ds(head, block), :]
                        for c in range(full // lanes):
                            line = u * unit + c * lines + q * block
                            to[:, c * lanes : (c + 1) * lanes] = ref[line : line + block, :].astype(f32)
                        far = q * block >= lines // 2
                        line = u * unit + (full // lanes) * lines + q * block - (lines // 2 if far else 0)
                        x = ref[line : line + block, :].astype(f32)
                        to[:, full:] = x[:, left:] if far else x[:, :left]


def on_device(query, cache, segments, groups, value_up, out_proj, targets):
    query_len, head_count, width = query.shape
    latent, vwidth = value_up.shape[1], value_up.shape[2]
    rows = query_len * head_count
    cache_len = cache.shape[0]
    half = head_count // 2
    seq_stages = stages_of(lax.axis_size("seq"), 2)
    head_stages = stages_of(lax.axis_size("heads"))
    pair = (1, 2)
    shape = jax.ShapeDtypeStruct
    vmem = pl.BlockSpec(memory_space=pltpu.VMEM)
    payload = shape((half + 1, query_len, vwidth), bf16)
    hbm = pl.BlockSpec(memory_space=pltpu.HBM)
    own, other, weights, stats, query_rows = call(
        forward_kernel,
        (
            payload,
            payload,
            shape((rows, cache_len), f32),
            shape((2, 2, query_len, lanes), f32),
            shape((rows, width), bf16),
        ),
        query.reshape(rows, width),
        cache,
        segments.reshape(1, cache_len),
        groups.reshape(query_len, 1),
        value_up,
        scratch=(
            pltpu.VMEM(value_up.shape, bf16),
            pltpu.VMEM((head_count, query_len, latent), bf16),
            pltpu.VMEM((2, half + 1, query_len, vwidth), bf16),
            pltpu.SemaphoreType.DMA,
        ),
        specs=[vmem] * 4 + [hbm],
        flops=2 * rows * (cache_len * (width + latent) + latent * vwidth),
        grant=46 << 20,
    )
    state = call(combine_kernel, payload, own, swap(other, "seq", pair, 1))
    for stage in seq_stages:
        state = call(combine_kernel, payload, *swap_all(state, "seq", stage), flops=waiting)
    state_got = swap(state, "seq", pair, 1)
    partial = call(
        project_kernel,
        shape(targets.shape, bf16),
        state,
        state_got,
        out_proj,
        scratch=(pltpu.VMEM((query_len, head_count * vwidth), bf16),),
        flops=2 * query_len * out_proj.size,
    )
    for stage in head_stages[:-1]:
        partial = call(partial_sum_kernel, shape(partial.shape, bf16), *swap_all(partial, "heads", stage))
    projected, own, other = call(
        functools.partial(residual_kernel, head_stages[-1]),
        (shape(targets.shape, f32), payload, payload),
        *swap_all(partial, "heads", head_stages[-1]),
        targets,
        out_proj,
        scratch=(pltpu.VMEM((2, half + 1, query_len, vwidth), bf16),),
        flops=2 * query_len * out_proj.size,
    )
    d_state = call(functools.partial(sum_kernel, pair), payload, own, swap(other, "seq", pair, 1))
    for stage in seq_stages:
        d_state = call(functools.partial(sum_kernel, stage), payload, *swap_all(d_state, "seq", stage), flops=waiting)
    d_got = swap(d_state, "seq", pair, 1)
    loss = jnp.sum(d_state[half].astype(f32)) / (query_len * targets.shape[1] * lax.axis_size("seq"))
    chunks = 1
    count = head_count // chunks
    units = shape((2, count // 4, query_len // 4 * 8 * width // lanes, lanes), bf16)
    wide = shape((count, query_len, cache_len), bf16)
    local = [
        call(
            functools.partial(backward_kernel, chunk),
            (units, wide, wide, shape((count, query_len, latent), bf16)),
            d_state,
            d_got,
            state,
            state_got,
            weights,
            stats,
            cache,
            value_up,
            flops=rows * (cache_len * (width + latent) + latent * vwidth),
            grant=10 << 20,
        )
        for chunk in range(chunks)
    ]
    pieces = [scatter_sum(x[0].reshape(2, -1, lanes), "seq", pair) for x in local]
    for stage in seq_stages:
        pieces = [scatter_sum(x.reshape(stage[1], -1, lanes), "seq", stage) for x in pieces]
    cache_part = None
    for chunk, (_, d_scores, probs, d_latent) in enumerate(local):
        d_scores = d_scores.reshape(-1, cache_len)
        span = query_rows.shape[0] // chunks
        held = query_rows[chunk * span : (chunk + 1) * span]
        key_part = jnp.einsum("rt,rc->ct", d_scores, held, preferred_element_type=f32)
        value_part = jnp.einsum(
            "rt,rc->ct", probs.reshape(-1, cache_len), d_latent.reshape(-1, latent), preferred_element_type=f32
        )
        part = jnp.concatenate([key_part[:latent] + value_part, key_part[latent:]], axis=0)
        cache_part = part if cache_part is None else cache_part + part
    cache_part = cache_part.astype(bf16)
    for stage in head_stages[::-1]:
        cache_part = cache_part.reshape(stage[1], cache_part.shape[0] // stage[1], cache_len)
        cache_part = scatter_sum(cache_part, "heads", stage)
    for stage in seq_stages[:0:-1]:
        pieces = [gather(x, "seq", stage).reshape(-1, lanes) for x in pieces]
    parts = []
    for x in pieces:
        own = swap_all(x, "seq", seq_stages[0])
        parts += own + [swap(p, "seq", pair, 1) for p in own]
    query_grad = call(
        functools.partial(final_kernel, seq_stages[0], chunks), shape(query.shape, f32), *parts
    )
    return projected, loss, query_grad, cache_part.T.astype(f32)


def solution(mesh):
    in_specs = (
        P(None, "heads", None),
        P("seq", None),
        P("seq"),
        P(),
        P("heads", None, None),
        P("heads", "seq"),
        P(None, "seq"),
    )
    out_specs = (P(None, "seq"), P(), P(None, "heads", None), P("seq", "heads"))

    return jax.shard_map(on_device, mesh=mesh, in_specs=in_specs, out_specs=out_specs, check_vma=False)
```
